32 devices in a mesh: pts: 8 (over y, x, core), wlk: 4 (over z).
Axes of the slice: x: 2, y: 2, z: 4, core: 2. Of those that a mesh axis runs over, the one named last changes fastest.
Arguments:
- green_half: bfloat16 [8, 400, 2400], P('wlk'), may hold values from -6 to 6
- collocation: bfloat16 [2400, 9600], P('wlk', 'pts'), may hold values from -0.125 to 0.125
- occupied: bfloat16 [9600, 400], P('pts'), may hold values from -0.0029296875 to 0.0029296875
- kernel: bfloat16 [9600, 9600], P('pts'), may hold values from 0 to 16, as said below
Outputs:
- potential: float32 [8, 9600], P('wlk', 'pts')
- coulomb_energy: float32 [8], P('wlk')
- exchange_energy: float32 [8], P('wlk')
The draws below stay inside these ranges and needn't reach their ends.
Inputs may be any that keep to these rules, and one draw needn't show every extreme that they name: kernel is symmetric and positive definite: kernel[p, q] equals kernel[q, p].
All inputs are finite; a program needn't handle non-finite values.
Results may differ from the reference program's by a relative error of at most 0.008.
Values may be sent and summed in bfloat16 or wider, within the bound.
A program may use at most 192 MiB of HBM per device.

```python
import jax
import jax.numpy as jnp
from jax import lax

ORB = 2400
ELEC = 400
RANK = 9600
W = 8


def draw_kernel(key, part):
    point_spots = jax.random.uniform(jax.random.fold_in(key, 3), (RANK, 3), jnp.float32, 0.0, 1.0)
    length = (10.0 / RANK) ** (1.0 / 3.0)
    squared = jnp.zeros((RANK, RANK), jnp.float32)
    for column in range(3):
        offset = point_spots[:, column][:, None] - point_spots[:, column][None, :]
        squared = squared + offset * offset
    distance = jnp.sqrt(squared)
    values = 6.0 * jnp.exp(-distance / length) + 1.5 * jnp.eye(RANK, dtype=jnp.float32)
    return values.astype(jnp.bfloat16)


def block_scale(own_key, extent, split, smallest, largest):
    level, own = 1.0, jax.random.fold_in(own_key, 6)
    for axis_at, shards_of in split:
        draws = jnp.exp(jax.random.uniform(jax.random.fold_in(own, axis_at), (shards_of,), jnp.float32, smallest / len(split), largest / len(split)))
        level = level * jnp.repeat(draws, extent[axis_at] // shards_of).reshape([-1 if axis == axis_at else 1 for axis in range(len(extent))])
    return level


def noise(rng, shape, scale, limit, split=(), held_as=jnp.bfloat16):
    values = scale * jax.random.normal(rng, shape, jnp.float32)
    if split:
        values = values * block_scale(rng, shape, split, -0.22, 0.18)
    return jnp.clip(values, -limit, limit).astype(held_as)


def setup_inputs(seed: int = 0) -> dict:
    arg_keys = jax.random.split(jax.random.key(seed), 5)
    return {
        "green_half": noise(arg_keys[0], (W, ELEC, ORB), 1.0, 6.0, ((0, 4),)),
        "collocation": noise(arg_keys[1], (ORB, RANK), ORB ** -0.5, 0.125, ((0, 4), (1, 8))),
        "occupied": noise(arg_keys[2], (RANK, ELEC), (RANK * ELEC) ** -0.5, 0.0029296875, ((0, 8),)),
        "kernel": draw_kernel(jax.random.fold_in(arg_keys[4], 71), 0),
    }


def reference(green_half, collocation, occupied, kernel):
    kernel_float = kernel.astype(jnp.float32)

    def one_walker(green_one):
        theta = jnp.dot(green_one, collocation, preferred_element_type=jnp.float32).astype(jnp.bfloat16)
        density = jnp.sum(theta.astype(jnp.float32) * occupied.T.astype(jnp.float32), axis=0)
        density_b = density.astype(jnp.bfloat16)
        potential = jnp.dot(kernel, density_b, preferred_element_type=jnp.float32)
        coulomb = 0.5 * jnp.sum(density * potential)
        cross = jnp.dot(theta.T, occupied.T, preferred_element_type=jnp.float32)
        exchange = -0.5 * jnp.sum(kernel_float * cross * cross.T)
        return potential, coulomb, exchange

    potential, coulomb, exchange = lax.map(one_walker, green_half)
    return potential, coulomb, exchange
```

```python
import functools

import jax
import jax.numpy as jnp
from jax import lax
from jax.experimental import pallas as pl
from jax.experimental.pallas import tpu as pltpu
from jax.sharding import PartitionSpec as P

CHUNK = 256
LANES = 128
MESH = pl.DeviceIdType.MESH
F32 = jnp.float32
BF16 = jnp.bfloat16


def body(
    bits_n, planes, chunks, frame, piece,
    green_ref, coll_ref, occ_ref, kern_ref,
    pot_ref, coul_ref, exch_ref,
    occ, gin, gs, xg, tht, thr, pht, thq, kal, kst, dens, dq, acc, pot, eall,
    load_sem, kload_sem, zsend, zrecv, psend, precv, tsend, trecv, dsend, drecv, esend, erecv,
):
    n = 1 << bits_n
    rows, elec = occ.shape
    walkers = tht.shape[0]
    orb = coll_ref.shape[0]
    steps = len(chunks)
    me = lax.axis_index("pts")
    z = lax.axis_index("wlk")
    bit = [(me // (1 << t)) % 2 for t in range(bits_n)]

    def peer(d):
        out = me
        for t in range(bits_n):
            if (d >> t) & 1:
                out = out + (1 << t) * (1 - 2 * bit[t])
        return out

    def remote(src, dst, send, recv, to):
        return pltpu.make_async_remote_copy(
            src_ref=src, dst_ref=dst, send_sem=send, recv_sem=recv, device_id=to, device_id_type=MESH
        )

    occ_load = pltpu.make_async_copy(occ_ref, occ, load_sem.at[0])
    occ_load.start()
    x_load = pltpu.make_async_copy(coll_ref, xg.at[z], load_sem.at[1])
    x_load.start()
    g_load = pltpu.make_async_copy(green_ref.at[0], gin, load_sem.at[2])
    g_load.start()

    pieces = []
    total = kern_ref.shape[1]
    for b in range(n):
        start = (rows * b) // LANES * LANES
        width = min(frame + LANES, total - start)
        for r in range(0, rows, piece):
            pieces.append((b, r, start, width, rows * b - start))

    def window(i):
        b, r, start, width, _ = pieces[i]
        return pltpu.make_async_copy(
            kern_ref.at[pl.ds(r, piece), pl.ds(start, width)],
            kst.at[i % 2, :, pl.ds(0, width)],
            kload_sem.at[i % 2],
        )

    window(0).start()
    window(1).start()

    def realign(i):
        b, r, _, width, shift = pieces[i]
        window(i).wait()
        have = min(frame, width - shift)
        kal[b, pl.ds(r, piece), pl.ds(0, have)] = kst[i % 2, :, shift : shift + have]
        if have < frame:
            kal[b, pl.ds(r, piece), pl.ds(have, frame - have)] = jnp.zeros((piece, frame - have), BF16)
        if i + 2 < len(pieces):
            window(i + 2).start()

    barrier = pltpu.get_barrier_semaphore()
    for d in range(1, n):
        pl.semaphore_signal(barrier, inc=1, device_id=(peer(d), z), device_id_type=MESH)

    @pl.when(z > 0)
    def _():
        pl.semaphore_signal(barrier, inc=1, device_id=(me, z - 1), device_id_type=MESH)

    @pl.when(z < planes - 1)
    def _():
        pl.semaphore_signal(barrier, inc=1, device_id=(me, z + 1), device_id_type=MESH)

    ends = (z == 0).astype(jnp.int32) + (z == planes - 1).astype(jnp.int32)
    pl.semaphore_wait(barrier, n - 1 + 2 - ends)

    def z_copy(way, s, k, own):
        lo, wide, _ = chunks[k]
        there = z + (1 if way else -1)
        src = coll_ref.at[:, pl.ds(lo, wide)] if own else xg.at[s, :, pl.ds(lo, wide)]
        return remote(
            src, xg.at[s, :, pl.ds(lo, wide)], zsend.at[way, s, k], zrecv.at[s, k], (me, there)
        )

    def z_own(k):
        @pl.when(z > 0)
        def _():
            z_copy(0, z, k, True).start()

        @pl.when(z < planes - 1)
        def _():
            z_copy(1, z, k, True).start()

    def z_pass(k, j):
        for way, ok, more, s in (
            (0, z + j < planes, z > 0, z + j),
            (1, z - j >= 0, z < planes - 1, z - j),
        ):
            @pl.when(ok)
            def _():
                z_copy(way, s, k, False).wait_recv()

                @pl.when(more)
                def _():
                    z_copy(way, s, k, False).start()

    def z_done(k):
        for j in range(planes):
            for way, ok, s in (
                (0, (z + j < planes) & (z > 0), z + j),
                (1, (z - j >= 0) & (z < planes - 1), z - j),
            ):
                @pl.when(ok)
                def _():
                    z_copy(way, s, k, j == 0).wait_send()

    def occ_copy(t, d):
        return remote(
            pht.at[d], pht.at[d ^ (1 << t)], psend.at[t, d], precv.at[d ^ (1 << t)], (peer(1 << t), z)
        )

    def th_copy(t, d, k):
        lo, _, wide = chunks[k]
        if d == 0:
            src = tht.at[1 - bit[t], :, pl.ds(lo, wide)]
        else:
            src = thq.at[d, :, pl.ds(lo, wide)]
        e = d ^ (1 << t)
        return remote(
            src, thq.at[e, :, pl.ds(lo, wide)], tsend.at[t, d, k], trecv.at[e, k], (peer(1 << t), z)
        )

    def d_copy(d, k):
        lo, _, wide = chunks[k]
        return remote(
            dq.at[0, :, pl.ds(lo, wide)], dq.at[d, :, pl.ds(lo, wide)],
            dsend.at[d, k], drecv.at[d, k], (peer(d), z),
        )

    z_own(0)
    if steps > 1:
        z_own(1)

    acc[...] = jnp.zeros_like(acc)
    pot[...] = jnp.zeros_like(pot)
    dens[...] = jnp.zeros_like(dens)
    dq[0] = jnp.zeros_like(dq[0])
    if rows < frame:
        for w in range(walkers):
            tht[w, :, pl.ds(rows, frame - rows)] = jnp.zeros((elec, frame - rows), BF16)
        pht[0, :, pl.ds(rows, frame - rows)] = jnp.zeros((elec, frame - rows), BF16)
    occ_load.wait()
    for lo, wide, _ in chunks:
        pht[0, :, pl.ds(lo, wide)] = occ[pl.ds(lo, wide), :].T

    chip_bits = list(range(1, bits_n))
    held = [0]
    sent = []
    plan = []
    for t in chip_bits + [0]:
        plan.append((t, list(held)))
        held = held + [d ^ (1 << t) for d in held]
    for t, _ in plan:
        occ_copy(t, 0).start()

    def occ_pass(step):
        t, deltas = plan[step]
        for d in deltas:
            e = d ^ (1 << t)
            occ_copy(t, d).wait_recv()
            for later, ds in plan[step + 1 :]:
                if e in ds:
                    occ_copy(later, e).start()

    for w in range(walkers):
        g_load.wait()
        for s in range(planes):
            gs[s, pl.ds(w * elec, elec), :] = gin[:, s * orb : (s + 1) * orb]
        if w + 1 < walkers:
            g_load = pltpu.make_async_copy(green_ref.at[w + 1], gin, load_sem.at[2])
            g_load.start()

    at = 0
    share = len(pieces) // 4
    for i in range(share):
        realign(i)
    at = share
    z_first = [1] if planes > 1 else []
    for j in z_first:
        z_pass(0, j)
    for step in range(len(plan) - 1):
        for i in range(at, at + share):
            realign(i)
        at += share
        occ_pass(step)
    for i in range(at, len(pieces)):
        realign(i)
    occ_pass(len(plan) - 1)

    th_plan = []
    held = [0]
    for t in list(reversed(chip_bits)) + [0]:
        th_plan.append((t, list(held)))
        held = held + [d ^ (1 << t) for d in held]

    def theta(k):
        lo, valid, wide = chunks[k]
        total = None
        for s in range(planes):
            part = jnp.dot(gs[s], xg[s, :, pl.ds(lo, valid)], preferred_element_type=F32)
            total = part if total is None else total + part
        for w in range(walkers):
            one = total[w * elec : (w + 1) * elec].astype(BF16)
            tht[w, :, pl.ds(lo, valid)] = one
        for w in range(walkers):
            turned = tht[w, :, pl.ds(lo, valid)]
            thr[w, pl.ds(lo, valid), :] = turned.T
            value = jnp.sum(
                turned.astype(F32) * pht[0, :, pl.ds(lo, valid)].astype(F32), axis=0, keepdims=True
            )
            dens[pl.ds(w, 1), pl.ds(lo, valid)] = value
        dq[0, pl.ds(0, 8), pl.ds(lo, wide)] = dens[pl.ds(0, 8), pl.ds(lo, wide)].astype(BF16)
        for t, _ in th_plan:
            th_copy(t, 0, k).start()
        for d in range(1, n):
            d_copy(d, k).start()

    def th_pass(k):
        for step, (t, deltas) in enumerate(th_plan[:-1]):
            for d in deltas:
                e = d ^ (1 << t)
                th_copy(t, d, k).wait_recv()
                for later, ds in th_plan[step + 1 :]:
                    if e in ds:
                        th_copy(later, e, k).start()

    def th_last(k):
        t, deltas = th_plan[-1]
        for d in deltas:
            th_copy(t, d, k).wait_recv()
        for d in range(1, n):
            d_copy(d, k).wait_recv()

    def fold(w, b, near_lhs, far_lhs, near_rhs, far_rhs, p0, pm, q0, qw, weight):
        near = jnp.dot(near_lhs, near_rhs, preferred_element_type=F32)
        far = jnp.dot(far_lhs, far_rhs, preferred_element_type=F32)
        term = near * far * kal[b, pl.ds(p0, pm), pl.ds(q0, qw)].astype(F32)
        acc[w, :, pl.ds(0, qw)] += weight * jnp.sum(term.reshape(pm // 8, 8, qw), axis=0)

    def exchange(k):
        lo, valid, wide = chunks[k]
        full = lo + valid

        @pl.loop(0, walkers)
        def _(w):
            if lo > 0:
                fold(w, me, thr[w, pl.ds(0, lo), :], occ[pl.ds(0, lo), :], pht[0, :, pl.ds(lo, wide)],
                     tht[w, :, pl.ds(lo, wide)], 0, lo, lo, wide, 2.0)
            fold(w, me, thr[w, pl.ds(lo, valid), :], occ[pl.ds(lo, valid), :], pht[0, :, pl.ds(lo, wide)],
                 tht[w, :, pl.ds(lo, wide)], lo, valid, lo, wide, 1.0)

        th_last(k)

        @pl.loop(1, n)
        def _(d):
            b = jnp.int32(0)
            w = jnp.int32(0)
            for t in range(bits_n):
                b = b + (1 << t) * ((bit[t] + d // (1 << t)) % 2)
                w = w + jnp.where(d // (1 << t) == 1, bit[t], 0)
            fold(w, b, thr[w, pl.ds(0, full), :], occ[pl.ds(0, full), :], pht[d, :, pl.ds(lo, wide)],
                 thq[d, :, pl.ds(lo, wide)], 0, full, lo, wide, 2.0)
            if k > 0:
                @pl.loop(0, k)
                def _(j):
                    q0 = pl.multiple_of(j * CHUNK, CHUNK)
                    fold(w, b, thr[w, pl.ds(lo, valid), :], occ[pl.ds(lo, valid), :],
                         pht[d, :, pl.ds(q0, CHUNK)], thq[d, :, pl.ds(q0, CHUNK)],
                         lo, valid, q0, CHUNK, 2.0)

        @pl.loop(0, n)
        def _(d):
            b = jnp.int32(0)
            for t in range(bits_n):
                b = b + (1 << t) * ((bit[t] + d // (1 << t)) % 2)
            pot[...] += lax.dot_general(
                kal[b, :, pl.ds(lo, wide)], dq[d, :, pl.ds(lo, wide)],
                (((1,), (1,)), ((), ())), preferred_element_type=F32,
            )

    for k in range(steps):
        for j in range(1, planes):
            if not (k == 0 and j in z_first):
                z_pass(k, j)
        if k + 2 < steps:
            z_own(k + 2)
        if k == 0:
            x_load.wait()
        theta(k)
        if k > 0:
            exchange(k - 1)
        th_pass(k)
    exchange(steps - 1)

    pot_rows = pot[...].T
    pot_ref[...] = pot_rows[:walkers, :]
    for w in range(walkers):
        eall[me, pl.ds(w, 1), :] = jnp.full((1, LANES), 0.5 * jnp.sum(dens[pl.ds(w, 1), pl.ds(0, rows)] * pot_rows[w : w + 1, :]), F32)
        eall[me, pl.ds(walkers + w, 1), :] = jnp.full((1, LANES), -0.5 * jnp.sum(acc[w]), F32)

    def e_copy(d):
        return remote(eall.at[me], eall.at[me], esend.at[d], erecv.at[d], (peer(d), z))

    def e_wait(d):
        return remote(eall.at[peer(d)], eall.at[peer(d)], esend.at[d], erecv.at[d], (peer(d), z))

    for d in range(1, n):
        e_copy(d).start()
    for d in range(1, n):
        e_wait(d).wait_recv()
    whole = eall[0]
    for b in range(1, n):
        whole = whole + eall[b]
    for w in range(walkers):
        coul_ref[w] = whole[w, 0]
        exch_ref[w] = whole[walkers + w, 0]

    for d in range(1, n):
        e_copy(d).wait_send()
    for t, deltas in plan:
        for d in deltas:
            occ_copy(t, d).wait_send()
    for k in range(steps):
        z_done(k)
        for t, deltas in th_plan:
            for d in deltas:
                th_copy(t, d, k).wait_send()
        for d in range(1, n):
            d_copy(d, k).wait_send()


def local(green_half, collocation, occupied, kernel):
    walkers, elec, _ = green_half.shape
    orb, rows = collocation.shape
    n = lax.axis_size("pts")
    planes = lax.axis_size("wlk")
    bits_n = n.bit_length() - 1
    frame = pl.cdiv(rows, LANES) * LANES
    chunks = []
    for lo in range(0, rows, CHUNK):
        chunks.append((lo, min(CHUNK, rows - lo), min(CHUNK, frame - lo)))
    steps = len(chunks)
    piece = max([r for r in range(16, 256, 16) if rows % r == 0] or [rows])
    anywhere = pl.BlockSpec(memory_space=pl.ANY)
    smem = pl.BlockSpec(memory_space=pltpu.SMEM)
    dma = pltpu.SemaphoreType.DMA
    potential, coulomb, exchange = pl.pallas_call(
        functools.partial(body, bits_n, planes, tuple(chunks), frame, piece),
        out_shape=(
            jax.ShapeDtypeStruct((walkers, rows), F32),
            jax.ShapeDtypeStruct((walkers,), F32),
            jax.ShapeDtypeStruct((walkers,), F32),
        ),
        in_specs=[anywhere] * 4,
        out_specs=(pl.BlockSpec(memory_space=pltpu.VMEM), smem, smem),
        scratch_shapes=[
            pltpu.VMEM((rows, elec), BF16),
            pltpu.VMEM((elec, green_half.shape[2]), BF16),
            pltpu.VMEM((planes, walkers * elec, orb), BF16),
            pltpu.VMEM((planes, orb, rows), BF16),
            pltpu.VMEM((walkers, elec, frame), BF16),
            pltpu.VMEM((walkers, rows, elec), BF16),
            pltpu.VMEM((n, elec, frame), BF16),
            pltpu.VMEM((n, elec, frame), BF16),
            pltpu.VMEM((n, rows, frame), BF16),
            pltpu.VMEM((2, piece, frame + LANES), BF16),
            pltpu.VMEM((8, frame), F32),
            pltpu.VMEM((n, 16, frame), BF16),
            pltpu.VMEM((walkers, 8, CHUNK), F32),
            pltpu.VMEM((rows, 16), F32),
            pltpu.VMEM((n, 8, LANES), F32),
            dma((3,)),
            dma((2,)),
            dma((2, planes, steps)),
            dma((planes, steps)),
            dma((bits_n, n)),
            dma((n,)),
            dma((bits_n, n, steps)),
            dma((n, steps)),
            dma((n, steps)),
            dma((n, steps)),
            dma((n,)),
            dma((n,)),
        ],
        compiler_params=pltpu.CompilerParams(
            collective_id=0, has_side_effects=True, vmem_limit_bytes=67043328
        ),
        name="energy",
    )(green_half, collocation, occupied, kernel)
    return potential, coulomb, exchange


def solution(mesh):
    placed = (P("wlk", None, None), P("wlk", "pts"), P("pts", None), P("pts", None))
    return jax.shard_map(
        local,
        mesh=mesh,
        in_specs=placed,
        out_specs=(P("wlk", "pts"), P("wlk"), P("wlk")),
        check_vma=False,
    )
```

```python
import functools

import jax
import jax.numpy as jnp
from jax import lax
from jax.experimental import pallas as pl
from jax.experimental.pallas import tpu as pltpu
from jax.sharding import PartitionSpec as P

CHUNK = 256
LANES = 128
MESH = pl.DeviceIdType.MESH
F32 = jnp.float32
BF16 = jnp.bfloat16


def body(
    bits_n, planes, chunks, frame, piece,
    green_ref, coll_ref, occ_ref, kern_ref,
    pot_ref, coul_ref, exch_ref,
    occ, gin, gs, xg, tht, thr, pht, thq, kal, kext, dens, dq, acc, pot, eall,
    load_sem, kload_sem, zsend, zrecv, psend, precv, tsend, trecv, dsend, drecv, esend, erecv,
):
    n = 1 << bits_n
    rows, elec = occ.shape
    walkers = tht.shape[0]
    orb = coll_ref.shape[0]
    steps = len(chunks)
    me = lax.axis_index("pts")
    z = lax.axis_index("wlk")
    bit = [(me // (1 << t)) % 2 for t in range(bits_n)]

    def peer(d):
        out = me
        for t in range(bits_n):
            if (d >> t) & 1:
                out = out + (1 << t) * (1 - 2 * bit[t])
        return out

    def remote(src, dst, send, recv, to):
        return pltpu.make_async_remote_copy(
            src_ref=src, dst_ref=dst, send_sem=send, recv_sem=recv, device_id=to, device_id_type=MESH
        )

    occ_load = pltpu.make_async_copy(occ_ref, pht.at[0], load_sem.at[0])
    occ_load.start()
    x_load = pltpu.make_async_copy(coll_ref, xg.at[z], load_sem.at[1])
    x_load.start()
    g_load = pltpu.make_async_copy(green_ref.at[0], gin, load_sem.at[2])
    g_load.start()

    windows = []
    spill = 0
    for b in range(n):
        start = (rows * b) // LANES * LANES
        shift = rows * b - start
        over = shift + rows > frame
        windows.append((start, min(frame, kern_ref.shape[1] - start), shift, spill if over else None))
        spill += over

    def window(b):
        start, width, _, extra = windows[b]
        copies = [
            pltpu.make_async_copy(
                kern_ref.at[:, pl.ds(start, width)], kal.at[b, :, pl.ds(0, width)], kload_sem.at[0, b]
            )
        ]
        if extra is not None:
            copies.append(
                pltpu.make_async_copy(
                    kern_ref.at[:, pl.ds(start + frame, LANES)], kext.at[extra], kload_sem.at[1, b]
                )
            )
        return copies

    for b in range(n):
        for copy in window(b):
            copy.start()

    def realign(b):
        _, width, shift, extra = windows[b]
        for copy in window(b):
            copy.wait()
        if shift > 0:
            @pl.loop(0, rows // piece)
            def _(i):
                r = pl.multiple_of(i * piece, piece)
                part = kal[b, pl.ds(r, piece), :]
                if extra is not None:
                    part = jnp.concatenate([part, kext[extra, pl.ds(r, piece), :]], axis=1)
                kal[b, pl.ds(r, piece), pl.ds(0, rows)] = part[:, shift : shift + rows]

    barrier = pltpu.get_barrier_semaphore()
    for d in range(1, n):
        pl.semaphore_signal(barrier, inc=1, device_id=(peer(d), z), device_id_type=MESH)

    @pl.when(z > 0)
    def _():
        pl.semaphore_signal(barrier, inc=1, device_id=(me, z - 1), device_id_type=MESH)

    @pl.when(z < planes - 1)
    def _():
        pl.semaphore_signal(barrier, inc=1, device_id=(me, z + 1), device_id_type=MESH)

    ends = (z == 0).astype(jnp.int32) + (z == planes - 1).astype(jnp.int32)
    pl.semaphore_wait(barrier, n - 1 + 2 - ends)

    def z_copy(way, s, k, own):
        lo, wide = chunks[k]
        there = z + (1 if way else -1)
        src = coll_ref.at[:, pl.ds(lo, wide)] if own else xg.at[s, :, pl.ds(lo, wide)]
        return remote(
            src, xg.at[s, :, pl.ds(lo, wide)], zsend.at[way, s, k], zrecv.at[s, k], (me, there)
        )

    def z_own(k):
        @pl.when(z > 0)
        def _():
            z_copy(0, z, k, True).start()

        @pl.when(z < planes - 1)
        def _():
            z_copy(1, z, k, True).start()

    def ways(j):
        return ((0, z + j < planes, z > 0, z + j), (1, z - j >= 0, z < planes - 1, z - j))

    def z_pass(k, j):
        for way, ok, more, s in ways(j):
            @pl.when(ok & more)
            def _():
                z_copy(way, s, k, False).wait_recv()
                z_copy(way, s, k, False).start()

    def z_take(k):
        for j in range(1, planes):
            for way, ok, more, s in ways(j):
                @pl.when(ok & jnp.logical_not(more))
                def _():
                    z_copy(way, s, k, False).wait_recv()

    def z_done(k):
        for j in range(planes):
            for way, ok, s in (
                (0, (z + j < planes) & (z > 0), z + j),
                (1, (z - j >= 0) & (z < planes - 1), z - j),
            ):
                @pl.when(ok)
                def _():
                    z_copy(way, s, k, j == 0).wait_send()

    def occ_copy(t, d):
        return remote(
            pht.at[d], pht.at[d ^ (1 << t)], psend.at[t, d], precv.at[d ^ (1 << t)], (peer(1 << t), z)
        )

    def th_copy(t, d, k):
        lo, wide = chunks[k]
        if d == 0:
            src = tht.at[1 - bit[t], :, pl.ds(lo, wide)]
        else:
            src = thq.at[d - 1, :, pl.ds(lo, wide)]
        e = d ^ (1 << t)
        return remote(
            src, thq.at[e - 1, :, pl.ds(lo, wide)], tsend.at[t, d, k], trecv.at[e, k], (peer(1 << t), z)
        )

    def d_copy(d, k):
        lo, wide = chunks[k]
        return remote(
            dq.at[0, :, pl.ds(lo, wide)], dq.at[d, :, pl.ds(lo, wide)],
            dsend.at[d, k], drecv.at[d, k], (peer(d), z),
        )

    z_own(0)
    if steps > 1:
        z_own(1)

    acc[...] = jnp.zeros_like(acc)
    pot[...] = jnp.zeros_like(pot)
    dens[...] = jnp.zeros_like(dens)
    occ_load.wait()
    for lo, wide in chunks:
        occ[pl.ds(lo, wide), :] = pht[0, :, pl.ds(lo, wide)].T

    chip_bits = list(range(1, bits_n))
    held = [0]
    sent = []
    plan = []
    for t in chip_bits + [0]:
        plan.append((t, list(held)))
        held = held + [d ^ (1 << t) for d in held]
    for t, _ in plan:
        occ_copy(t, 0).start()

    def occ_pass(step):
        t, deltas = plan[step]
        for d in deltas:
            e = d ^ (1 << t)
            occ_copy(t, d).wait_recv()
            for later, ds in plan[step + 1 :]:
                if e in ds:
                    occ_copy(later, e).start()

    for w in range(walkers):
        g_load.wait()
        for s in range(planes):
            gs[s, pl.ds(w * elec, elec), :] = gin[:, s * orb : (s + 1) * orb]
        if w + 1 < walkers:
            g_load = pltpu.make_async_copy(green_ref.at[w + 1], gin, load_sem.at[2])
            g_load.start()

    th_plan = []
    held = [0]
    for t in list(reversed(chip_bits)) + [0]:
        th_plan.append((t, list(held)))
        held = held + [d ^ (1 << t) for d in held]

    def theta(k):
        lo, valid = chunks[k]
        total = None
        for s in range(planes):
            part = jnp.dot(gs[s], xg[s, :, pl.ds(lo, valid)], preferred_element_type=F32)
            total = part if total is None else total + part
        for w in range(walkers):
            one = total[w * elec : (w + 1) * elec].astype(BF16)
            tht[w, :, pl.ds(lo, valid)] = one
        for w in range(walkers):
            turned = tht[w, :, pl.ds(lo, valid)]
            thr[w, pl.ds(lo, valid), :] = turned.T
            value = jnp.sum(
                turned.astype(F32) * pht[0, :, pl.ds(lo, valid)].astype(F32), axis=0, keepdims=True
            )
            dens[pl.ds(w, 1), pl.ds(lo, valid)] = value
        dq[0, :, pl.ds(lo, valid)] = dens[:, pl.ds(lo, valid)].astype(BF16)
        for t, _ in th_plan:
            th_copy(t, 0, k).start()
        for d in range(1, n):
            d_copy(d, k).start()

    arrivals = []
    for t, deltas in th_plan[-1:] + th_plan[:-1]:
        for d in deltas:
            if t > 0 or d == 0:
                arrivals.append((t, d))
    for d in th_plan[-1][1]:
        if d > 0:
            arrivals.append((0, d))
    order = [d ^ (1 << t) for t, d in arrivals]

    arrived = set()

    def arrive(i, k):
        if (i, k) in arrived:
            return
        arrived.add((i, k))
        t, d = arrivals[i]
        e = order[i]
        th_copy(t, d, k).wait_recv()
        for later, ds in th_plan:
            if e in ds:
                th_copy(later, e, k).start()
        d_copy(e, k).wait_recv()

    def lanes_to(x, width):
        out = x[:, :width]
        for at in range(width, x.shape[1], width):
            out = out + x[:, at : at + width]
        return out

    def spread(d, kf, p0, pm, q0, qw):
        for w in range(walkers):
            u = kf * dq[d, pl.ds(w, 1), pl.ds(q0, qw)].astype(F32)
            if qw > LANES and qw % LANES:
                cut = qw // LANES * LANES
                pot[w, pl.ds(p0, pm), :] += lanes_to(u[:, :cut], LANES)
                pot[w, pl.ds(p0, pm), pl.ds(0, qw - cut)] += u[:, cut:]
            else:
                part = lanes_to(u, min(LANES, qw))
                pot[w, pl.ds(p0, pm), pl.ds(0, min(LANES, qw))] += part

    def fold(w, b, d, far_rhs, p0, pm, q0, qw, weight):
        near = jnp.dot(thr[w, pl.ds(p0, pm), :], pht[d, :, pl.ds(q0, qw)], preferred_element_type=F32)
        far = jnp.dot(occ[pl.ds(p0, pm), :], far_rhs, preferred_element_type=F32)
        kf = kal[b, pl.ds(p0, pm), pl.ds(q0, qw)].astype(F32)
        term = near * far * kf
        term = lanes_to(jnp.sum(term.reshape(pm // 8, 8, qw), axis=0), min(qw, CHUNK))
        acc[w, :, pl.ds(0, min(qw, CHUNK))] += weight * term
        return kf

    def pair(d):
        b = jnp.int32(0)
        w = jnp.int32(0)
        for t in range(bits_n):
            b = b + (1 << t) * ((bit[t] + d // (1 << t)) % 2)
            w = w + jnp.where(d // (1 << t) == 1, bit[t], 0)
        return b, w

    def exchange_old(k):
        lo, wide = chunks[k]
        if k == 0:
            return

        @pl.loop(1, n)
        def _(d):
            b, w = pair(d)
            kf = fold(w, b, d, thq[d - 1, :, pl.ds(0, lo)], lo, wide, 0, lo, 2.0)
            spread(d, kf, lo, wide, 0, lo)

    def exchange_own(k):
        lo, wide = chunks[k]

        @pl.loop(0, walkers)
        def _(w):
            rhs = tht[w, :, pl.ds(lo, wide)]
            if lo > 0:
                fold(w, me, 0, rhs, 0, lo, lo, wide, 2.0)
            fold(w, me, 0, rhs, lo, wide, lo, wide, 1.0)

        spread(0, kal[me, :, pl.ds(lo, wide)].astype(F32), 0, rows, lo, wide)

    def exchange_new(k, services):
        lo, wide = chunks[k]
        full = lo + wide

        @pl.loop(0, n - 1)
        def _(i):
            d = jnp.int32(0)
            for j in range(n - 1):
                d = d + jnp.where(i == j, order[j], 0)

                @pl.when(i == j)
                def _():
                    arrive(j, k)
                    for serve in services.get(j, ()):
                        serve()

            b, w = pair(d)
            kf = fold(w, b, d, thq[d - 1, :, pl.ds(lo, wide)], 0, full, lo, wide, 2.0)
            spread(d, kf, 0, full, lo, wide)

    def near_pass(k):
        if k < steps:
            z_pass(k, 1)

    def far_pass(k):
        if k < steps:
            for j in range(2, planes):
                z_pass(k, j)

    def own_send(k):
        if 1 < k < steps:
            z_own(k)

    def first_arrivals(k):
        for i, (t, d) in enumerate(arrivals):
            if t > 0 and d == 0:
                arrive(i, k)

    def exchange_all(k, services):
        exchange_old(k)
        exchange_own(k)
        exchange_new(k, services)

    near_pass(0)
    for b in range(n):
        realign(b)
    near_pass(1)
    own_send(2)
    occ_pass(0)
    far_pass(0)
    z_take(0)
    x_load.wait()
    theta(0)
    far_pass(1)
    near_pass(2)
    own_send(3)
    first_arrivals(0)
    for step in range(1, len(plan)):
        occ_pass(step)
    for k in range(1, steps):
        if k == steps - 1:
            exchange_old(k - 1)
            exchange_own(k - 1)
            first_arrivals(k - 1)
        z_take(k)
        theta(k)
        far_pass(k + 1)
        near_pass(k + 2)
        own_send(k + 3)
        if k == 1 and k < steps - 1:
            exchange_all(0, {n - 2: [functools.partial(first_arrivals, 1)]})
        if k == steps - 1:
            exchange_new(k - 1, {n - 3: [functools.partial(first_arrivals, k)]})
        elif k < steps - 2:
            exchange_all(k, {})
    exchange_old(steps - 1)
    exchange_own(steps - 1)
    exchange_new(steps - 1, {})

    pot_rows = []
    for w in range(walkers):
        pot_rows.append(jnp.sum(pot[w].T, axis=0, keepdims=True))
        pot_ref[pl.ds(w, 1), :] = pot_rows[w]
    for w in range(walkers):
        eall[me, pl.ds(w, 1), :] = jnp.full((1, LANES), 0.5 * jnp.sum(dens[pl.ds(w, 1), :] * pot_rows[w]), F32)
        eall[me, pl.ds(walkers + w, 1), :] = jnp.full((1, LANES), -0.5 * jnp.sum(acc[w]), F32)

    def e_copy(d):
        return remote(eall.at[me], eall.at[me], esend.at[d], erecv.at[d], (peer(d), z))

    def e_wait(d):
        return remote(eall.at[peer(d)], eall.at[peer(d)], esend.at[d], erecv.at[d], (peer(d), z))

    for d in range(1, n):
        e_copy(d).start()
    for d in range(1, n):
        e_wait(d).wait_recv()
    whole = eall[0]
    for b in range(1, n):
        whole = whole + eall[b]
    for w in range(walkers):
        coul_ref[w] = whole[w, 0]
        exch_ref[w] = whole[walkers + w, 0]

    for d in range(1, n):
        e_copy(d).wait_send()
    for t, deltas in plan:
        for d in deltas:
            occ_copy(t, d).wait_send()
    for k in range(steps):
        z_done(k)
        for t, deltas in th_plan:
            for d in deltas:
                th_copy(t, d, k).wait_send()
        for d in range(1, n):
            d_copy(d, k).wait_send()


def local(green_half, collocation, occupied, kernel):
    walkers, elec, _ = green_half.shape
    orb, rows = collocation.shape
    n = lax.axis_size("pts")
    planes = lax.axis_size("wlk")
    bits_n = n.bit_length() - 1
    frame = pl.cdiv(rows, LANES) * LANES
    chunks = []
    for lo in range(0, rows, CHUNK):
        chunks.append((lo, min(CHUNK, rows - lo)))
    steps = len(chunks)
    spills = max(1, sum((rows * b) % LANES + rows > frame for b in range(n)))
    piece = max([r for r in range(16, 256, 16) if rows % r == 0] or [rows])
    anywhere = pl.BlockSpec(memory_space=pl.ANY)
    smem = pl.BlockSpec(memory_space=pltpu.SMEM)
    dma = pltpu.SemaphoreType.DMA
    potential, coulomb, exchange = pl.pallas_call(
        functools.partial(body, bits_n, planes, tuple(chunks), frame, piece),
        out_shape=(
            jax.ShapeDtypeStruct((walkers, rows), F32),
            jax.ShapeDtypeStruct((walkers,), F32),
            jax.ShapeDtypeStruct((walkers,), F32),
        ),
        in_specs=[anywhere] * 4,
        out_specs=(pl.BlockSpec(memory_space=pltpu.VMEM), smem, smem),
        scratch_shapes=[
            pltpu.VMEM((rows, elec), BF16),
            pltpu.VMEM((elec, green_half.shape[2]), BF16),
            pltpu.VMEM((planes, walkers * elec, orb), BF16),
            pltpu.VMEM((planes, orb, rows), BF16),
            pltpu.VMEM((walkers, elec, rows), BF16),
            pltpu.VMEM((walkers, rows, elec), BF16),
            pltpu.VMEM((n, elec, rows), BF16),
            pltpu.VMEM((n - 1, elec, rows), BF16),
            pltpu.VMEM((n, rows, frame), BF16),
            pltpu.VMEM((spills, rows, LANES), BF16),
            pltpu.VMEM((8, rows), F32),
            pltpu.VMEM((n, 8, rows), BF16),
            pltpu.VMEM((walkers, 8, CHUNK), F32),
            pltpu.VMEM((walkers, rows, LANES), F32),
            pltpu.VMEM((n, 8, LANES), F32),
            dma((3,)),
            dma((2, n)),
            dma((2, planes, steps)),
            dma((planes, steps)),
            dma((bits_n, n)),
            dma((n,)),
            dma((bits_n, n, steps)),
            dma((n, steps)),
            dma((n, steps)),
            dma((n, steps)),
            dma((n,)),
            dma((n,)),
        ],
        compiler_params=pltpu.CompilerParams(
            collective_id=0, has_side_effects=True, vmem_limit_bytes=67043328
        ),
        name="energy",
    )(green_half, collocation, occupied.T, kernel)
    return potential, coulomb, exchange


def solution(mesh):
    placed = (P("wlk", None, None), P("wlk", "pts"), P("pts", None), P("pts", None))
    return jax.shard_map(
        local,
        mesh=mesh,
        in_specs=placed,
        out_specs=(P("wlk", "pts"), P("wlk"), P("wlk")),
        check_vma=False,
    )
```

```python
import functools

import jax
import jax.numpy as jnp
from jax import lax
from jax.experimental import pallas as pl
from jax.experimental.pallas import tpu as pltpu
from jax.sharding import PartitionSpec as P

CHUNK = 256
LANES = 128
MESH = pl.DeviceIdType.MESH
F32 = jnp.float32
BF16 = jnp.bfloat16


def body(
    bits_n, planes, chunks, helped, frame, piece,
    green_ref, coll_ref, occ_ref, kern_ref,
    out_ref,
    occ, gin, gs, gs2, tout, xg, tht, thr, pht, thq, kal, kext, dens, dq, acc, pot, eall,
    load_sem, kload_sem, zsend, zrecv, psend, precv, tsend, trecv, dsend, drecv, esend, erecv, gsend, grecv, hsend, hrecv,
):
    n = 1 << bits_n
    rows, elec = occ.shape
    walkers = tht.shape[0]
    orb = coll_ref.shape[0]
    steps = len(chunks)
    me = lax.axis_index("pts")
    z = lax.axis_index("wlk")
    bit = [(me // (1 << t)) % 2 for t in range(bits_n)]

    def peer(d):
        out = me
        for t in range(bits_n):
            if (d >> t) & 1:
                out = out + (1 << t) * (1 - 2 * bit[t])
        return out

    def remote(src, dst, send, recv, to):
        return pltpu.make_async_remote_copy(
            src_ref=src, dst_ref=dst, send_sem=send, recv_sem=recv, device_id=to, device_id_type=MESH
        )

    occ_load = pltpu.make_async_copy(occ_ref, pht.at[0], load_sem.at[0])
    occ_load.start()
    x_load = pltpu.make_async_copy(coll_ref, xg.at[z], load_sem.at[1])
    x_load.start()
    slab = gin.shape[1]
    slabs = [(w, r) for w in range(walkers) for r in range(0, elec, slab)]

    def g_load(i):
        w, r = slabs[i]
        return pltpu.make_async_copy(green_ref.at[w, pl.ds(r, slab), :], gin.at[i % 2], load_sem.at[2 + i % 2])

    g_load(0).start()
    if len(slabs) > 1:
        g_load(1).start()

    windows = []
    spill = 0
    for b in range(n):
        start = (rows * b) // LANES * LANES
        shift = rows * b - start
        over = shift + rows > frame
        windows.append((start, min(frame, kern_ref.shape[1] - start), shift, spill if over else None))
        spill += over

    def window(b):
        start, width, _, extra = windows[b]
        copies = [
            pltpu.make_async_copy(
                kern_ref.at[:, pl.ds(start, width)], kal.at[b, :, pl.ds(0, width)], kload_sem.at[0, b]
            )
        ]
        if extra is not None:
            copies.append(
                pltpu.make_async_copy(
                    kern_ref.at[:, pl.ds(start + frame, LANES)], kext.at[extra], kload_sem.at[1, b]
                )
            )
        return copies

    def realign(b):
        _, width, shift, extra = windows[b]
        for copy in window(b):
            copy.wait()
        if shift > 0:
            @pl.loop(0, rows // piece)
            def _(i):
                r = pl.multiple_of(i * piece, piece)
                part = kal[b, pl.ds(r, piece), :]
                if extra is not None:
                    part = jnp.concatenate([part, kext[extra, pl.ds(r, piece), :]], axis=1)
                kal[b, pl.ds(r, piece), pl.ds(0, rows)] = part[:, shift : shift + rows]

    barrier = pltpu.get_barrier_semaphore()
    for d in range(1, n):
        pl.semaphore_signal(barrier, inc=1, device_id=(peer(d), z), device_id_type=MESH)

    @pl.when(z > 0)
    def _():
        pl.semaphore_signal(barrier, inc=1, device_id=(me, z - 1), device_id_type=MESH)

    @pl.when(z < planes - 1)
    def _():
        pl.semaphore_signal(barrier, inc=1, device_id=(me, z + 1), device_id_type=MESH)

    ends = (z == 0).astype(jnp.int32) + (z == planes - 1).astype(jnp.int32)
    pl.semaphore_wait(barrier, n - 1 + 2 - ends)

    def z_copy(way, s, k, own):
        lo, wide = chunks[k]
        there = z + (1 if way else -1)
        src = coll_ref.at[:, pl.ds(lo, wide)] if own else xg.at[s, :, pl.ds(lo, wide)]
        return remote(
            src, xg.at[s, :, pl.ds(lo, wide)], zsend.at[way, s, k], zrecv.at[s, k], (me, there)
        )

    first_helped = min(helped, default=steps)
    at_end = (z == 0) | (z == planes - 1)
    helping = (z == 1) | (z == planes - 2)

    def low(k):
        return 1 if k in helped else 0

    def z_own(k):
        @pl.when(z > low(k))
        def _():
            z_copy(0, z, k, True).start()

        @pl.when(z < planes - 1 - low(k))
        def _():
            z_copy(1, z, k, True).start()

    def ways(j, k):
        return (
            (0, z + j < planes, z > low(k), z + j),
            (1, z - j >= 0, z < planes - 1 - low(k), z - j),
        )

    def z_pass(k, j):
        for way, ok, more, s in ways(j, k):
            @pl.when(ok & more)
            def _():
                z_copy(way, s, k, False).wait_recv()
                z_copy(way, s, k, False).start()

    def z_take(k):
        for j in range(1, planes):
            for way, ok, more, s in ways(j, k):
                need = ok & jnp.logical_not(more)
                if k in helped:
                    need = need & jnp.logical_not(at_end | helping)

                @pl.when(need)
                def _():
                    z_copy(way, s, k, False).wait_recv()

    def z_done(k):
        for j in range(planes):
            for way, ok, more, s in ways(j, k):
                @pl.when(ok & more)
                def _():
                    z_copy(way, s, k, j == 0).wait_send()

    end_to = z + 1 - 2 * (z // (planes - 1)) if planes > 1 else z
    help_to = z - 1 + 2 * ((z + 1) // (planes - 1)) if planes > 1 else z
    half = walkers * elec // 2

    def g_part(ref, s, c):
        return ref.at[s, pl.ds(pl.multiple_of(c * half, 16), half), :]

    def g_out(s):
        return remote(
            g_part(gs, s, bit[0]), g_part(gs2, s, bit[0]), gsend.at[0, s], grecv.at[0, s], (me, end_to)
        )

    def g_share(s):
        return remote(
            g_part(gs2, s, bit[0]), g_part(gs2, s, bit[0]), gsend.at[1, s], grecv.at[1, s], (peer(1), z)
        )

    def g_got(s):
        return remote(
            g_part(gs2, s, 1 - bit[0]), g_part(gs2, s, 1 - bit[0]), gsend.at[1, s], grecv.at[1, s], (peer(1), z)
        )

    def g_first():
        if helped:
            @pl.when(helping)
            def _():
                for s in range(planes):
                    g_out(s).wait_recv()
                    g_share(s).start()

    def h_copy(k):
        lo, wide = chunks[k]
        base = chunks[first_helped][0]
        return remote(
            tout.at[:, :, pl.ds(lo - base, wide)], tht.at[:, :, pl.ds(lo, wide)],
            hsend.at[k - first_helped], hrecv.at[k - first_helped], (me, help_to),
        )

    def help_end(k):
        if k in helped:
            lo, wide = chunks[k]
            base = chunks[first_helped][0]

            @pl.when(helping)
            def _():
                for s in range(planes):
                    g_got(s).wait_recv()
                for j in range(1, planes):
                    for way, ok, more, s in ways(j, k):
                        @pl.when(ok & jnp.logical_not(more))
                        def _():
                            z_copy(way, s, k, False).wait_recv()
                total = None
                for s in range(planes):
                    part = jnp.dot(gs2[s], xg[s, :, pl.ds(lo, wide)], preferred_element_type=F32)
                    total = part if total is None else total + part
                for w in range(walkers):
                    tout[w, :, pl.ds(lo - base, wide)] = total[w * elec : (w + 1) * elec].astype(BF16)
                h_copy(k).start()

    def occ_copy(t, d):
        return remote(
            pht.at[d], pht.at[d ^ (1 << t)], psend.at[t, d], precv.at[d ^ (1 << t)], (peer(1 << t), z)
        )

    def th_copy(t, d, k):
        lo, wide = chunks[k]
        if d == 0:
            src = tht.at[1 - bit[t], :, pl.ds(lo, wide)]
        else:
            src = thq.at[d - 1, :, pl.ds(lo, wide)]
        e = d ^ (1 << t)
        return remote(
            src, thq.at[e - 1, :, pl.ds(lo, wide)], tsend.at[t, d, k], trecv.at[e, k], (peer(1 << t), z)
        )

    def d_copy(d, k):
        lo, wide = chunks[k]
        return remote(
            dq.at[0, :, pl.ds(lo, wide)], dq.at[d, :, pl.ds(lo, wide)],
            dsend.at[d, k], drecv.at[d, k], (peer(d), z),
        )

    z_own(0)
    if steps > 1:
        z_own(1)
    if helped:
        @pl.when(at_end)
        def _():
            for k in range(2, steps):
                z_own(k)

    for b in range(n):
        for copy in window(b):
            copy.start()

    acc[...] = jnp.zeros_like(acc)
    pot[...] = jnp.zeros_like(pot)
    dens[...] = jnp.zeros_like(dens)
    occ_load.wait()
    for lo, wide in chunks:
        occ[pl.ds(lo, wide), :] = pht[0, :, pl.ds(lo, wide)].T

    chip_bits = list(range(1, bits_n))
    held = [0]
    sent = []
    plan = []
    for t in chip_bits + [0]:
        plan.append((t, list(held)))
        held = held + [d ^ (1 << t) for d in held]
    for t, _ in plan:
        occ_copy(t, 0).start()

    def occ_pass(step):
        t, deltas = plan[step]
        for d in deltas:
            e = d ^ (1 << t)
            occ_copy(t, d).wait_recv()
            for later, ds in plan[step + 1 :]:
                if e in ds:
                    occ_copy(later, e).start()

    for i, (w, r) in enumerate(slabs):
        g_load(i).wait()
        for s in range(planes):
            gs[s, pl.ds(w * elec + r, slab), :] = gin[i % 2, :, s * orb : (s + 1) * orb]
        if i + 2 < len(slabs):
            g_load(i + 2).start()
    if helped:
        @pl.when(at_end)
        def _():
            for s in range(planes):
                g_out(s).start()

    th_plan = []
    held = [0]
    for t in list(reversed(chip_bits)) + [0]:
        th_plan.append((t, list(held)))
        held = held + [d ^ (1 << t) for d in held]

    def theta(k):
        lo, valid = chunks[k]

        def make():
            total = None
            for s in range(planes):
                part = jnp.dot(gs[s], xg[s, :, pl.ds(lo, valid)], preferred_element_type=F32)
                total = part if total is None else total + part
            for w in range(walkers):
                tht[w, :, pl.ds(lo, valid)] = total[w * elec : (w + 1) * elec].astype(BF16)

        if k in helped:
            pl.when(jnp.logical_not(at_end))(make)

            @pl.when(at_end)
            def _():
                remote(
                    tht.at[:, :, pl.ds(lo, valid)], tht.at[:, :, pl.ds(lo, valid)],
                    hsend.at[k - first_helped], hrecv.at[k - first_helped], (me, end_to),
                ).wait_recv()
        else:
            make()
        for w in range(walkers):
            turned = tht[w, :, pl.ds(lo, valid)]
            thr[w, pl.ds(lo, valid), :] = turned.T
            value = jnp.sum(
                turned.astype(F32) * pht[0, :, pl.ds(lo, valid)].astype(F32), axis=0, keepdims=True
            )
            dens[pl.ds(w, 1), pl.ds(lo, valid)] = value
        dq[0, :, pl.ds(lo, valid)] = dens[:, pl.ds(lo, valid)].astype(BF16)
        for t, _ in th_plan:
            th_copy(t, 0, k).start()
        for d in range(1, n):
            d_copy(d, k).start()

    arrivals = []
    for t, deltas in th_plan[-1:] + th_plan[:-1]:
        for d in deltas:
            if t > 0 or d == 0:
                arrivals.append((t, d))
    for d in th_plan[-1][1]:
        if d > 0:
            arrivals.append((0, d))
    order = [d ^ (1 << t) for t, d in arrivals]

    arrived = set()

    def arrive(i, k):
        if (i, k) in arrived:
            return
        arrived.add((i, k))
        t, d = arrivals[i]
        e = order[i]
        th_copy(t, d, k).wait_recv()
        for later, ds in th_plan:
            if e in ds:
                th_copy(later, e, k).start()
        d_copy(e, k).wait_recv()

    def lanes_to(x, width):
        out = x[:, :width]
        for at in range(width, x.shape[1], width):
            out = out + x[:, at : at + width]
        return out

    def spread(d, kf, p0, pm, q0, qw):
        for w in range(walkers):
            u = kf * dq[d, pl.ds(w, 1), pl.ds(q0, qw)].astype(F32)
            if qw > LANES and qw % LANES:
                cut = qw // LANES * LANES
                pot[w, pl.ds(p0, pm), :] += lanes_to(u[:, :cut], LANES)
                pot[w, pl.ds(p0, pm), pl.ds(0, qw - cut)] += u[:, cut:]
            else:
                part = lanes_to(u, min(LANES, qw))
                pot[w, pl.ds(p0, pm), pl.ds(0, min(LANES, qw))] += part

    def fold(w, b, d, far_rhs, p0, pm, q0, qw, weight):
        near = jnp.dot(thr[w, pl.ds(p0, pm), :], pht[d, :, pl.ds(q0, qw)], preferred_element_type=F32)
        far = jnp.dot(occ[pl.ds(p0, pm), :], far_rhs, preferred_element_type=F32)
        kf = kal[b, pl.ds(p0, pm), pl.ds(q0, qw)].astype(F32)
        term = near * far * kf
        term = lanes_to(jnp.sum(term.reshape(pm // 8, 8, qw), axis=0), min(qw, CHUNK))
        acc[w, :, pl.ds(0, min(qw, CHUNK))] += weight * term
        return kf

    def pair(d):
        b = jnp.int32(0)
        w = jnp.int32(0)
        for t in range(bits_n):
            b = b + (1 << t) * ((bit[t] + d // (1 << t)) % 2)
            w = w + jnp.where(d // (1 << t) == 1, bit[t], 0)
        return b, w

    def exchange_old(k):
        lo, wide = chunks[k]
        if k == 0:
            return

        @pl.loop(1, n)
        def _(d):
            b, w = pair(d)
            kf = fold(w, b, d, thq[d - 1, :, pl.ds(0, lo)], lo, wide, 0, lo, 2.0)
            spread(d, kf, lo, wide, 0, lo)

    def exchange_own(k):
        lo, wide = chunks[k]

        @pl.loop(0, walkers)
        def _(w):
            rhs = tht[w, :, pl.ds(lo, wide)]
            if lo > 0:
                fold(w, me, 0, rhs, 0, lo, lo, wide, 2.0)
            fold(w, me, 0, rhs, lo, wide, lo, wide, 1.0)

        for p0 in range(0, rows, 2 * CHUNK):
            pm = min(2 * CHUNK, rows - p0)
            spread(0, kal[me, pl.ds(p0, pm), pl.ds(lo, wide)].astype(F32), p0, pm, lo, wide)

    def exchange_new(k, services):
        lo, wide = chunks[k]
        full = lo + wide

        @pl.loop(0, n - 1)
        def _(i):
            d = jnp.int32(0)
            for j in range(n - 1):
                d = d + jnp.where(i == j, order[j], 0)

                @pl.when(i == j)
                def _():
                    arrive(j, k)
                    for serve in services.get(j, ()):
                        serve()

            b, w = pair(d)
            for p0 in range(0, full, 2 * CHUNK):
                pm = min(2 * CHUNK, full - p0)
                kf = fold(w, b, d, thq[d - 1, :, pl.ds(lo, wide)], p0, pm, lo, wide, 2.0)
                spread(d, kf, p0, pm, lo, wide)

    def near_pass(k):
        if k < steps:
            z_pass(k, 1)

    def far_pass(k):
        if k < steps:
            for j in range(2, planes):
                z_pass(k, j)

    def own_send(k):
        if 1 < k < steps:
            if helped:
                pl.when(jnp.logical_not(at_end))(lambda: z_own(k))
            else:
                z_own(k)

    def first_arrivals(k):
        for i, (t, d) in enumerate(arrivals):
            if t > 0 and d == 0:
                arrive(i, k)

    def exchange_all(k, services):
        exchange_old(k)
        exchange_own(k)
        exchange_new(k, services)

    near_pass(0)
    for b in range(n):
        realign(b)
    near_pass(1)
    own_send(2)
    occ_pass(0)
    far_pass(0)
    z_take(0)
    x_load.wait()
    theta(0)
    far_pass(1)
    near_pass(2)
    own_send(3)
    first_arrivals(0)
    for step in range(1, len(plan)):
        occ_pass(step)
    for k in range(1, steps):
        if k == steps - 1:
            exchange_old(k - 1)
            exchange_own(k - 1)
            first_arrivals(k - 1)
        z_take(k)
        theta(k)
        far_pass(k + 1)
        near_pass(k + 2)
        own_send(k + 3)
        if k == 1 and k < steps - 1:
            exchange_all(0, {n - 2: [functools.partial(first_arrivals, 1)]})
        if k == steps - 1:
            exchange_new(k - 1, {n - 3: [functools.partial(first_arrivals, k)]})
        elif k == steps - 3 and helped:
            exchange_old(k)
            exchange_own(k)
            first_arrivals(k)
            g_first()
            help_end(steps - 1)
            exchange_new(k, {})
        elif k < steps - 2:
            exchange_all(k, {})
    exchange_old(steps - 1)
    exchange_own(steps - 1)
    exchange_new(steps - 1, {})

    pot_rows = []
    for w in range(walkers):
        pot_rows.append(jnp.sum(pot[w].T, axis=0, keepdims=True))
        out_ref[pl.ds(w, 1), pl.ds(0, rows)] = pot_rows[w]
    for w in range(walkers):
        eall[me, pl.ds(w, 1), :] = jnp.full((1, LANES), 0.5 * jnp.sum(dens[pl.ds(w, 1), :] * pot_rows[w]), F32)
        eall[me, pl.ds(walkers + w, 1), :] = jnp.full((1, LANES), -0.5 * jnp.sum(acc[w]), F32)

    def e_copy(d):
        return remote(eall.at[me], eall.at[me], esend.at[d], erecv.at[d], (peer(d), z))

    def e_wait(d):
        return remote(eall.at[peer(d)], eall.at[peer(d)], esend.at[d], erecv.at[d], (peer(d), z))

    for d in range(1, n):
        e_copy(d).start()
    for d in range(1, n):
        e_wait(d).wait_recv()
    whole = eall[0]
    for b in range(1, n):
        whole = whole + eall[b]
    out_ref[:, pl.ds(frame, LANES)] = whole[: 2 * walkers]

    for d in range(1, n):
        e_copy(d).wait_send()
    for t, deltas in plan:
        for d in deltas:
            occ_copy(t, d).wait_send()
    if helped:
        @pl.when(at_end)
        def _():
            for s in range(planes):
                g_out(s).wait_send()

        @pl.when(helping)
        def _():
            for s in range(planes):
                g_share(s).wait_send()
            for k in helped:
                h_copy(k).wait_send()

    for k in range(steps):
        z_done(k)
        for t, deltas in th_plan:
            for d in deltas:
                th_copy(t, d, k).wait_send()
        for d in range(1, n):
            d_copy(d, k).wait_send()


def local(green_half, collocation, occupied, kernel):
    walkers, elec, _ = green_half.shape
    orb, rows = collocation.shape
    n = lax.axis_size("pts")
    planes = lax.axis_size("wlk")
    bits_n = n.bit_length() - 1
    frame = pl.cdiv(rows, LANES) * LANES
    chunks = []
    for lo in range(0, rows, CHUNK):
        chunks.append((lo, min(CHUNK, rows - lo)))
    steps = len(chunks)
    helped = (steps - 1,) if planes >= 4 and steps >= 4 and walkers * elec % 32 == 0 else ()
    late = chunks[helped[0]][0] if helped else 0
    slab = max([r for r in range(16, 96, 16) if elec % r == 0] or [elec])
    spills = max(1, sum((rows * b) % LANES + rows > frame for b in range(n)))
    piece = max([r for r in range(16, 256, 16) if rows % r == 0] or [rows])
    anywhere = pl.BlockSpec(memory_space=pl.ANY)
    dma = pltpu.SemaphoreType.DMA
    out = pl.pallas_call(
        functools.partial(body, bits_n, planes, tuple(chunks), helped, frame, piece),
        out_shape=jax.ShapeDtypeStruct((2 * walkers, frame + LANES), F32),
        in_specs=[anywhere] * 4,
        out_specs=pl.BlockSpec(memory_space=pltpu.VMEM),
        scratch_shapes=[
            pltpu.VMEM((rows, elec), BF16),
            pltpu.VMEM((2, slab, green_half.shape[2]), BF16),
            pltpu.VMEM((planes, walkers * elec, orb), BF16),
            pltpu.VMEM((planes, walkers * elec, orb) if helped else (1, 16, LANES), BF16),
            pltpu.VMEM((walkers, elec, rows - late) if helped else (1, 16, LANES), BF16),
            pltpu.VMEM((planes, orb, rows), BF16),
            pltpu.VMEM((walkers, elec, rows), BF16),
            pltpu.VMEM((walkers, rows, elec), BF16),
            pltpu.VMEM((n, elec, rows), BF16),
            pltpu.VMEM((n - 1, elec, rows), BF16),
            pltpu.VMEM((n, rows, frame), BF16),
            pltpu.VMEM((spills, rows, LANES), BF16),
            pltpu.VMEM((8, rows), F32),
            pltpu.VMEM((n, 8, rows), BF16),
            pltpu.VMEM((walkers, 8, CHUNK), F32),
            pltpu.VMEM((walkers, rows, LANES), F32),
            pltpu.VMEM((n, 8, LANES), F32),
            dma((4,)),
            dma((2, n)),
            dma((2, planes, steps)),
            dma((planes, steps)),
            dma((bits_n, n)),
            dma((n,)),
            dma((bits_n, n, steps)),
            dma((n, steps)),
            dma((n, steps)),
            dma((n, steps)),
            dma((n,)),
            dma((n,)),
            dma((2, planes)),
            dma((2, planes)),
            dma((steps,)),
            dma((steps,)),
        ],
        compiler_params=pltpu.CompilerParams(
            collective_id=0, has_side_effects=True, vmem_limit_bytes=67043328
        ),
        name="energy",
    )(green_half, collocation, occupied.T, kernel)
    return out[:walkers, :rows], out[:walkers, frame], out[walkers:, frame]


def solution(mesh):
    placed = (P("wlk", None, None), P("wlk", "pts"), P("pts", None), P("pts", None))
    return jax.shard_map(
        local,
        mesh=mesh,
        in_specs=placed,
        out_specs=(P("wlk", "pts"), P("wlk"), P("wlk")),
        check_vma=False,
    )
```

```python
import functools

import jax
import jax.numpy as jnp
from jax import lax
from jax.experimental import pallas as pl
from jax.experimental.pallas import tpu as pltpu
from jax.sharding import PartitionSpec as P

CHUNK = 256
LANES = 128
MESH = pl.DeviceIdType.MESH
F32 = jnp.float32
BF16 = jnp.bfloat16


def body(
    bits_n, planes, chunks, helped, frame, piece,
    green_ref, coll_ref, occ_ref, kern_ref,
    out_ref,
    occ, gin, gs, gs2, tout, xg, tht, thr, pht, thq, kal, kext, dens, dq, acc, pot, eall,
    load_sem, kload_sem, zsend, zrecv, psend, precv, tsend, trecv, dsend, drecv, esend, erecv, gsend, grecv, hsend, hrecv,
):
    n = 1 << bits_n
    rows, elec = occ.shape
    walkers = tht.shape[0]
    orb = coll_ref.shape[0]
    steps = len(chunks)
    me = lax.axis_index("pts")
    z = lax.axis_index("wlk")
    bit = [(me // (1 << t)) % 2 for t in range(bits_n)]

    def peer(d):
        out = me
        for t in range(bits_n):
            if (d >> t) & 1:
                out = out + (1 << t) * (1 - 2 * bit[t])
        return out

    def remote(src, dst, send, recv, to):
        return pltpu.make_async_remote_copy(
            src_ref=src, dst_ref=dst, send_sem=send, recv_sem=recv, device_id=to, device_id_type=MESH
        )

    occ_load = pltpu.make_async_copy(occ_ref, pht.at[0], load_sem.at[0])
    occ_load.start()
    x_load = pltpu.make_async_copy(coll_ref, xg.at[z], load_sem.at[1])
    x_load.start()
    slab = gin.shape[1]
    slabs = [(w, r) for w in range(walkers) for r in range(0, elec, slab)]

    def g_load(i):
        w, r = slabs[i]
        return pltpu.make_async_copy(green_ref.at[w, pl.ds(r, slab), :], gin.at[i % 2], load_sem.at[2 + i % 2])

    g_load(0).start()
    if len(slabs) > 1:
        g_load(1).start()

    windows = []
    spill = 0
    for b in range(n):
        start = (rows * b) // LANES * LANES
        shift = rows * b - start
        over = shift + rows > frame
        windows.append((start, min(frame, kern_ref.shape[1] - start), shift, spill if over else None))
        spill += over

    def window(b):
        start, width, _, extra = windows[b]
        copies = [
            pltpu.make_async_copy(
                kern_ref.at[:, pl.ds(start, width)], kal.at[b, :, pl.ds(0, width)], kload_sem.at[0, b]
            )
        ]
        if extra is not None:
            copies.append(
                pltpu.make_async_copy(
                    kern_ref.at[:, pl.ds(start + frame, LANES)], kext.at[extra], kload_sem.at[1, b]
                )
            )
        return copies

    def realign(b):
        _, width, shift, extra = windows[b]
        for copy in window(b):
            copy.wait()
        if shift > 0:
            @pl.loop(0, rows // piece)
            def _(i):
                r = pl.multiple_of(i * piece, piece)
                part = kal[b, pl.ds(r, piece), :]
                if extra is not None:
                    part = jnp.concatenate([part, kext[extra, pl.ds(r, piece), :]], axis=1)
                kal[b, pl.ds(r, piece), pl.ds(0, rows)] = part[:, shift : shift + rows]

    barrier = pltpu.get_barrier_semaphore()
    for d in range(1, n):
        pl.semaphore_signal(barrier, inc=1, device_id=(peer(d), z), device_id_type=MESH)

    @pl.when(z > 0)
    def _():
        pl.semaphore_signal(barrier, inc=1, device_id=(me, z - 1), device_id_type=MESH)

    @pl.when(z < planes - 1)
    def _():
        pl.semaphore_signal(barrier, inc=1, device_id=(me, z + 1), device_id_type=MESH)

    ends = (z == 0).astype(jnp.int32) + (z == planes - 1).astype(jnp.int32)
    pl.semaphore_wait(barrier, n - 1 + 2 - ends)

    def z_copy(way, s, k, own):
        lo, wide = chunks[k]
        there = z + (1 if way else -1)
        src = coll_ref.at[:, pl.ds(lo, wide)] if own else xg.at[s, :, pl.ds(lo, wide)]
        return remote(
            src, xg.at[s, :, pl.ds(lo, wide)], zsend.at[way, s, k], zrecv.at[s, k], (me, there)
        )

    first_helped = min(helped, default=steps)
    at_end = (z == 0) | (z == planes - 1)
    helping = (z == 1) | (z == planes - 2)

    def low(k):
        return 1 if k in helped else 0

    def z_own(k):
        @pl.when(z > low(k))
        def _():
            z_copy(0, z, k, True).start()

        @pl.when(z < planes - 1 - low(k))
        def _():
            z_copy(1, z, k, True).start()

    def ways(j, k):
        return (
            (0, z + j < planes, z > low(k), z + j),
            (1, z - j >= 0, z < planes - 1 - low(k), z - j),
        )

    def z_pass(k, j):
        for way, ok, more, s in ways(j, k):
            @pl.when(ok & more)
            def _():
                z_copy(way, s, k, False).wait_recv()
                z_copy(way, s, k, False).start()

    def z_take(k):
        for j in range(1, planes):
            for way, ok, more, s in ways(j, k):
                need = ok & jnp.logical_not(more)
                if k in helped:
                    need = need & jnp.logical_not(at_end | helping)

                @pl.when(need)
                def _():
                    z_copy(way, s, k, False).wait_recv()

    def z_done(k):
        for j in range(planes):
            for way, ok, more, s in ways(j, k):
                @pl.when(ok & more)
                def _():
                    z_copy(way, s, k, j == 0).wait_send()

    end_to = z + 1 - 2 * (z // (planes - 1)) if planes > 1 else z
    help_to = z - 1 + 2 * ((z + 1) // (planes - 1)) if planes > 1 else z
    half = walkers * elec // 2

    def g_part(ref, s, c):
        return ref.at[s, pl.ds(pl.multiple_of(c * half, 16), half), :]

    def g_out(s):
        return remote(
            g_part(gs, s, bit[0]), g_part(gs2, s, bit[0]), gsend.at[0, s], grecv.at[0, s], (me, end_to)
        )

    def g_share(s):
        return remote(
            g_part(gs2, s, bit[0]), g_part(gs2, s, bit[0]), gsend.at[1, s], grecv.at[1, s], (peer(1), z)
        )

    def g_got(s):
        return remote(
            g_part(gs2, s, 1 - bit[0]), g_part(gs2, s, 1 - bit[0]), gsend.at[1, s], grecv.at[1, s], (peer(1), z)
        )

    def g_first():
        if helped:
            @pl.when(helping)
            def _():
                for s in range(planes):
                    g_out(s).wait_recv()
                    g_share(s).start()

    def h_copy(k):
        lo, wide = chunks[k]
        base = chunks[first_helped][0]
        return remote(
            tout.at[:, :, pl.ds(lo - base, wide)], tht.at[:, :, pl.ds(lo, wide)],
            hsend.at[k - first_helped], hrecv.at[k - first_helped], (me, help_to),
        )

    def help_end(k):
        if k in helped:
            lo, wide = chunks[k]
            base = chunks[first_helped][0]

            @pl.when(helping)
            def _():
                for s in range(planes):
                    g_got(s).wait_recv()
                for j in range(1, planes):
                    for way, ok, more, s in ways(j, k):
                        @pl.when(ok & jnp.logical_not(more))
                        def _():
                            z_copy(way, s, k, False).wait_recv()
                total = None
                for s in range(planes):
                    part = jnp.dot(gs2[s], xg[s, :, pl.ds(lo, wide)], preferred_element_type=F32)
                    total = part if total is None else total + part
                for w in range(walkers):
                    tout[w, :, pl.ds(lo - base, wide)] = total[w * elec : (w + 1) * elec].astype(BF16)
                h_copy(k).start()

    def occ_copy(t, d):
        return remote(
            pht.at[d], pht.at[d ^ (1 << t)], psend.at[t, d], precv.at[d ^ (1 << t)], (peer(1 << t), z)
        )

    def th_copy(t, d, k):
        lo, wide = chunks[k]
        if d == 0:
            src = tht.at[1 - bit[t], :, pl.ds(lo, wide)]
        else:
            src = thq.at[d - 1, :, pl.ds(lo, wide)]
        e = d ^ (1 << t)
        return remote(
            src, thq.at[e - 1, :, pl.ds(lo, wide)], tsend.at[t, d, k], trecv.at[e, k], (peer(1 << t), z)
        )

    def d_copy(d, k):
        lo, wide = chunks[k]
        return remote(
            dq.at[0, :, pl.ds(lo, wide)], dq.at[d, :, pl.ds(lo, wide)],
            dsend.at[d, k], drecv.at[d, k], (peer(d), z),
        )

    z_own(0)
    if steps > 1:
        z_own(1)
    if helped:
        @pl.when(at_end)
        def _():
            for k in range(2, steps):
                z_own(k)

    occ_load.wait()
    acc[...] = jnp.zeros_like(acc)
    pot[...] = jnp.zeros_like(pot)
    dens[...] = jnp.zeros_like(dens)
    chip_bits = list(range(1, bits_n))
    held = [0]
    sent = []
    plan = []
    for t in chip_bits + [0]:
        plan.append((t, list(held)))
        held = held + [d ^ (1 << t) for d in held]
    for t, _ in plan:
        occ_copy(t, 0).start()
    for b in range(n):
        for copy in window(b):
            copy.start()
    for lo, wide in chunks:
        occ[pl.ds(lo, wide), :] = pht[0, :, pl.ds(lo, wide)].T

    def occ_pass(step):
        t, deltas = plan[step]
        for d in deltas:
            e = d ^ (1 << t)
            occ_copy(t, d).wait_recv()
            for later, ds in plan[step + 1 :]:
                if e in ds:
                    occ_copy(later, e).start()

    for i, (w, r) in enumerate(slabs):
        g_load(i).wait()
        for s in range(planes):
            gs[s, pl.ds(w * elec + r, slab), :] = gin[i % 2, :, s * orb : (s + 1) * orb]
        if i + 2 < len(slabs):
            g_load(i + 2).start()
    if helped:
        @pl.when(at_end)
        def _():
            for s in range(planes):
                g_out(s).start()

    th_plan = []
    held = [0]
    for t in list(reversed(chip_bits)) + [0]:
        th_plan.append((t, list(held)))
        held = held + [d ^ (1 << t) for d in held]

    def theta(k):
        lo, valid = chunks[k]

        def make():
            total = None
            for s in range(planes):
                part = jnp.dot(gs[s], xg[s, :, pl.ds(lo, valid)], preferred_element_type=F32)
                total = part if total is None else total + part
            for w in range(walkers):
                tht[w, :, pl.ds(lo, valid)] = total[w * elec : (w + 1) * elec].astype(BF16)

        if k in helped:
            pl.when(jnp.logical_not(at_end))(make)

            @pl.when(at_end)
            def _():
                remote(
                    tht.at[:, :, pl.ds(lo, valid)], tht.at[:, :, pl.ds(lo, valid)],
                    hsend.at[k - first_helped], hrecv.at[k - first_helped], (me, end_to),
                ).wait_recv()
        else:
            make()
        for w in range(walkers):
            thr[w, pl.ds(lo, valid), :] = tht[w, :, pl.ds(lo, valid)].T
        for t, _ in th_plan:
            th_copy(t, 0, k).start()
        for w in range(walkers):
            turned = tht[w, :, pl.ds(lo, valid)]
            value = jnp.sum(
                turned.astype(F32) * pht[0, :, pl.ds(lo, valid)].astype(F32), axis=0, keepdims=True
            )
            dens[pl.ds(w, 1), pl.ds(lo, valid)] = value
        dq[0, :, pl.ds(lo, valid)] = dens[:, pl.ds(lo, valid)].astype(BF16)
        for d in range(1, n):
            d_copy(d, k).start()

    arrivals = []
    for t, deltas in th_plan[-1:] + th_plan[:-1]:
        for d in deltas:
            if t > 0 or d == 0:
                arrivals.append((t, d))
    for d in th_plan[-1][1]:
        if d > 0:
            arrivals.append((0, d))
    order = [d ^ (1 << t) for t, d in arrivals]

    arrived = set()

    def arrive(i, k):
        if (i, k) in arrived:
            return
        arrived.add((i, k))
        t, d = arrivals[i]
        e = order[i]
        th_copy(t, d, k).wait_recv()
        for later, ds in th_plan:
            if e in ds:
                th_copy(later, e, k).start()
        d_copy(e, k).wait_recv()

    def lanes_to(x, width):
        out = x[:, :width]
        for at in range(width, x.shape[1], width):
            out = out + x[:, at : at + width]
        return out

    def spread(d, kf, p0, pm, q0, qw):
        for w in range(walkers):
            u = kf * dq[d, pl.ds(w, 1), pl.ds(q0, qw)].astype(F32)
            if qw > LANES and qw % LANES:
                cut = qw // LANES * LANES
                pot[w, pl.ds(p0, pm), :] += lanes_to(u[:, :cut], LANES)
                pot[w, pl.ds(p0, pm), pl.ds(0, qw - cut)] += u[:, cut:]
            else:
                part = lanes_to(u, min(LANES, qw))
                pot[w, pl.ds(p0, pm), pl.ds(0, min(LANES, qw))] += part

    def fold(w, b, d, far_rhs, p0, pm, q0, qw, weight):
        near = jnp.dot(thr[w, pl.ds(p0, pm), :], pht[d, :, pl.ds(q0, qw)], preferred_element_type=F32)
        far = jnp.dot(occ[pl.ds(p0, pm), :], far_rhs, preferred_element_type=F32)
        kf = kal[b, pl.ds(p0, pm), pl.ds(q0, qw)].astype(F32)
        term = near * far * kf
        term = lanes_to(jnp.sum(term.reshape(pm // 8, 8, qw), axis=0), min(qw, CHUNK))
        acc[w, :, pl.ds(0, min(qw, CHUNK))] += weight * term
        return kf

    def pair(d):
        b = jnp.int32(0)
        w = jnp.int32(0)
        for t in range(bits_n):
            b = b + (1 << t) * ((bit[t] + d // (1 << t)) % 2)
            w = w + jnp.where(d // (1 << t) == 1, bit[t], 0)
        return b, w

    def exchange_old(k, upto=None):
        lo, wide = chunks[k]
        upto = lo if upto is None else upto
        if upto == 0:
            return

        @pl.loop(1, n)
        def _(d):
            b, w = pair(d)
            kf = fold(w, b, d, thq[d - 1, :, pl.ds(0, upto)], lo, wide, 0, upto, 2.0)
            spread(d, kf, lo, wide, 0, upto)

    def exchange_own(k):
        lo, wide = chunks[k]

        @pl.loop(0, walkers)
        def _(w):
            rhs = tht[w, :, pl.ds(lo, wide)]
            if lo > 0:
                fold(w, me, 0, rhs, 0, lo, lo, wide, 2.0)
            fold(w, me, 0, rhs, lo, wide, lo, wide, 1.0)

        for p0 in range(0, rows, 2 * CHUNK):
            pm = min(2 * CHUNK, rows - p0)
            spread(0, kal[me, pl.ds(p0, pm), pl.ds(lo, wide)].astype(F32), p0, pm, lo, wide)

    def exchange_new(k, services, full=None):
        lo, wide = chunks[k]
        full = lo + wide if full is None else full

        @pl.loop(0, n - 1)
        def _(i):
            d = jnp.int32(0)
            for j in range(n - 1):
                d = d + jnp.where(i == j, order[j], 0)

                @pl.when(i == j)
                def _():
                    arrive(j, k)
                    for serve in services.get(j, ()):
                        serve()

            b, w = pair(d)
            for p0 in range(0, full, 2 * CHUNK):
                pm = min(2 * CHUNK, full - p0)
                kf = fold(w, b, d, thq[d - 1, :, pl.ds(lo, wide)], p0, pm, lo, wide, 2.0)
                spread(d, kf, p0, pm, lo, wide)

    def near_pass(k):
        if k < steps:
            z_pass(k, 1)

    def far_pass(k):
        if k < steps:
            for j in range(2, planes):
                z_pass(k, j)

    def own_send(k):
        if 1 < k < steps:
            if helped:
                pl.when(jnp.logical_not(at_end))(lambda: z_own(k))
            else:
                z_own(k)

    def first_arrivals(k):
        for i, (t, d) in enumerate(arrivals):
            if t > 0 and d == 0:
                arrive(i, k)

    def exchange_all(k, services):
        exchange_old(k)
        exchange_own(k)
        exchange_new(k, services)

    near_pass(0)
    for b in range(n):
        realign(b)
    near_pass(1)
    own_send(2)
    occ_pass(0)
    far_pass(0)
    z_take(0)
    x_load.wait()
    theta(0)
    far_pass(1)
    near_pass(2)
    own_send(3)
    first_arrivals(0)
    for step in range(1, len(plan)):
        occ_pass(step)
    for k in range(1, steps):
        if k == steps - 1:
            exchange_old(k - 1)
            exchange_own(k - 1)
            first_arrivals(k - 1)
        z_take(k)
        theta(k)
        far_pass(k + 1)
        near_pass(k + 2)
        own_send(k + 3)
        if k == 1 and k < steps - 1:
            exchange_all(0, {n - 2: [functools.partial(first_arrivals, 1)]})
        if k == steps - 1:
            exchange_old(k, chunks[k - 1][0])
            exchange_own(k)
            exchange_new(k - 1, {n // 2: [functools.partial(first_arrivals, k)]}, rows)
        elif k == steps - 3 and helped:
            exchange_old(k)
            exchange_own(k)
            first_arrivals(k)
            g_first()
            help_end(steps - 1)
            exchange_new(k, {})
        elif k < steps - 2:
            exchange_all(k, {})
    if steps == 1:
        exchange_own(0)
    exchange_new(steps - 1, {})

    pot_rows = []
    for w in range(walkers):
        pot_rows.append(jnp.sum(pot[w].T, axis=0, keepdims=True))
        out_ref[pl.ds(w, 1), pl.ds(0, rows)] = pot_rows[w]
    for w in range(walkers):
        eall[me, pl.ds(w, 1), :] = jnp.full((1, LANES), 0.5 * jnp.sum(dens[pl.ds(w, 1), :] * pot_rows[w]), F32)
        eall[me, pl.ds(walkers + w, 1), :] = jnp.full((1, LANES), -0.5 * jnp.sum(acc[w]), F32)

    def e_copy(d):
        return remote(eall.at[me], eall.at[me], esend.at[d], erecv.at[d], (peer(d), z))

    def e_wait(d):
        return remote(eall.at[peer(d)], eall.at[peer(d)], esend.at[d], erecv.at[d], (peer(d), z))

    for d in range(1, n):
        e_copy(d).start()
    for d in range(1, n):
        e_wait(d).wait_recv()
    whole = eall[0]
    for b in range(1, n):
        whole = whole + eall[b]
    out_ref[:, pl.ds(frame, LANES)] = whole[: 2 * walkers]

    for d in range(1, n):
        e_copy(d).wait_send()
    for t, deltas in plan:
        for d in deltas:
            occ_copy(t, d).wait_send()
    if helped:
        @pl.when(at_end)
        def _():
            for s in range(planes):
                g_out(s).wait_send()

        @pl.when(helping)
        def _():
            for s in range(planes):
                g_share(s).wait_send()
            for k in helped:
                h_copy(k).wait_send()

    for k in range(steps):
        z_done(k)
        for t, deltas in th_plan:
            for d in deltas:
                th_copy(t, d, k).wait_send()
        for d in range(1, n):
            d_copy(d, k).wait_send()


def local(green_half, collocation, occupied, kernel):
    walkers, elec, _ = green_half.shape
    orb, rows = collocation.shape
    n = lax.axis_size("pts")
    planes = lax.axis_size("wlk")
    bits_n = n.bit_length() - 1
    frame = pl.cdiv(rows, LANES) * LANES
    chunks = []
    for lo in range(0, rows, CHUNK):
        chunks.append((lo, min(CHUNK, rows - lo)))
    steps = len(chunks)
    helped = (steps - 1,) if planes >= 4 and steps >= 4 and walkers * elec % 32 == 0 else ()
    late = chunks[helped[0]][0] if helped else 0
    slab = max([r for r in range(16, 96, 16) if elec % r == 0] or [elec])
    spills = max(1, sum((rows * b) % LANES + rows > frame for b in range(n)))
    piece = max([r for r in range(16, 256, 16) if rows % r == 0] or [rows])
    anywhere = pl.BlockSpec(memory_space=pl.ANY)
    dma = pltpu.SemaphoreType.DMA
    out = pl.pallas_call(
        functools.partial(body, bits_n, planes, tuple(chunks), helped, frame, piece),
        out_shape=jax.ShapeDtypeStruct((2 * walkers, frame + LANES), F32),
        in_specs=[anywhere] * 4,
        out_specs=pl.BlockSpec(memory_space=pltpu.VMEM),
        scratch_shapes=[
            pltpu.VMEM((rows, elec), BF16),
            pltpu.VMEM((2, slab, green_half.shape[2]), BF16),
            pltpu.VMEM((planes, walkers * elec, orb), BF16),
            pltpu.VMEM((planes, walkers * elec, orb) if helped else (1, 16, LANES), BF16),
            pltpu.VMEM((walkers, elec, rows - late) if helped else (1, 16, LANES), BF16),
            pltpu.VMEM((planes, orb, rows), BF16),
            pltpu.VMEM((walkers, elec, rows), BF16),
            pltpu.VMEM((walkers, rows, elec), BF16),
            pltpu.VMEM((n, elec, rows), BF16),
            pltpu.VMEM((n - 1, elec, rows), BF16),
            pltpu.VMEM((n, rows, frame), BF16),
            pltpu.VMEM((spills, rows, LANES), BF16),
            pltpu.VMEM((8, rows), F32),
            pltpu.VMEM((n, 8, rows), BF16),
            pltpu.VMEM((walkers, 8, CHUNK), F32),
            pltpu.VMEM((walkers, rows, LANES), F32),
            pltpu.VMEM((n, 8, LANES), F32),
            dma((4,)),
            dma((2, n)),
            dma((2, planes, steps)),
            dma((planes, steps)),
            dma((bits_n, n)),
            dma((n,)),
            dma((bits_n, n, steps)),
            dma((n, steps)),
            dma((n, steps)),
            dma((n, steps)),
            dma((n,)),
            dma((n,)),
            dma((2, planes)),
            dma((2, planes)),
            dma((steps,)),
            dma((steps,)),
        ],
        compiler_params=pltpu.CompilerParams(
            collective_id=0, has_side_effects=True, vmem_limit_bytes=67043328
        ),
        name="energy",
    )(green_half, collocation, occupied.T, kernel)
    return out[:walkers, :rows], out[:walkers, frame], out[walkers:, frame]


def solution(mesh):
    placed = (P("wlk", None, None), P("wlk", "pts"), P("pts", None), P("pts", None))
    return jax.shard_map(
        local,
        mesh=mesh,
        in_specs=placed,
        out_specs=(P("wlk", "pts"), P("wlk"), P("wlk")),
        check_vma=False,
    )
```
